32 devices in a mesh: dp: 2 (over x), tp2: 4 (over z), tp: 4 (over y, core).
Axes of the slice: x: 2, y: 2, z: 4, core: 2. Of those that a mesh axis runs over, the one named last changes fastest.
Arguments:
- attn_out: bfloat16 [32768, 5120], P('dp', 'tp'), parts along dimension 0
- w_out: bfloat16 [5120, 5120], P('tp', 'tp2')
- residual: bfloat16 [32768, 5120], P(('dp', 'tp'), 'tp2'), parts along dimension 0
- norm_gain: float32 [5120], P('tp2')
Outputs:
- output 1: bfloat16 [32768, 5120], P(('dp', 'tp'), 'tp2'), parts along dimension 0
- output 2: bfloat16 [32768, 5120], P(('dp', 'tp'), 'tp2'), parts along dimension 0
There are 2 independent parts. The reference program is written for one: setup_inputs(seed, part) draws one part's arguments, and reference() takes and returns one part's arrays. A program takes and returns all parts, laid end to end along the dimension named above; an argument that names none is the same for every part.
All inputs are finite; a program needn't handle non-finite values.
Results may differ from the reference program's by a relative error of at most 0.00720159.
Values are sent between devices in bfloat16 or wider.
A program may use at most 1 GiB of HBM per device.

```python
import jax
import jax.numpy as jnp
from jax import lax

TOKENS = 16384
D = 5120
HEADS = 40
HEAD = 128
TP = 4
EPS_NORM = 1e-6


def setup_inputs(seed: int = 0, part: int = 0) -> dict:
    attn_width = HEADS * HEAD
    root_key = jax.random.key(seed)
    key_attn, key_w, key_res, key_gain = jax.random.split(root_key, 4)
    attn_vals = jax.random.normal(jax.random.fold_in(key_attn, part), (TOKENS, attn_width), jnp.float32)
    w_vals = jax.random.normal(key_w, (attn_width, D), jnp.float32) * (attn_width ** -0.5)
    res_vals = jax.random.normal(jax.random.fold_in(key_res, part), (TOKENS, D), jnp.float32)
    gain_vals = 1.0 + 0.3 * jax.random.normal(key_gain, (D,), jnp.float32)
    return {"attn_out": attn_vals.astype(jnp.bfloat16), "w_out": w_vals.astype(jnp.bfloat16), "residual": res_vals.astype(jnp.bfloat16), "norm_gain": gain_vals}


def reference(attn_out, w_out, residual, norm_gain):
    attn_width = attn_out.shape[1]
    shard_cols = attn_width // TP
    attn_shards = attn_out.reshape(TOKENS, TP, shard_cols).transpose(1, 0, 2)
    w_shards = w_out.reshape(TP, shard_cols, D)

    def add_shard(running, shard_pair):
        attn_blk, w_blk = shard_pair
        block_prod = jnp.dot(attn_blk, w_blk, preferred_element_type=jnp.float32).astype(jnp.bfloat16)
        return running + block_prod.astype(jnp.float32), None

    y_sum, _ = lax.scan(add_shard, jnp.zeros((TOKENS, D), jnp.float32), (attn_shards, w_shards))
    hidden = residual.astype(jnp.float32) + y_sum
    mean_sq = jnp.mean(hidden * hidden, axis=-1, keepdims=True)
    normed = hidden * lax.rsqrt(mean_sq + EPS_NORM) * norm_gain
    return hidden.astype(jnp.bfloat16), normed.astype(jnp.bfloat16)
```

```python
import functools

import jax
import jax.numpy as jnp
from jax import lax
from jax.experimental import pallas as pl
from jax.experimental.pallas import tpu as pltpu
from jax.sharding import PartitionSpec as P

EPS_NORM = 1e-6
MESH = pl.DeviceIdType.MESH
F32, BF16 = jnp.float32, jnp.bfloat16

NCH, NU, NY, NE = 64, 30, 30, 4
NV = NCH - NU
LOOK = 3
TILE = 128
LOCAL = 256


def gather_matmul(a, w, res, h, ss_out, asib, arem, wbuf, abuf, sbuf, rbuf, ss_own, ss_all,
                  ld, own_w, sib_recv, sib_send, y_recv, y_send, z_recv, z_send, e_recv, e_send, w_recv, w_send, ss_recv, ss_send):
    x, z, t = lax.axis_index("dp"), lax.axis_index("tp2"), lax.axis_index("tp")
    rows, width = h.shape
    depth = w.shape[0]
    half = depth // 2
    ch = rows // NCH
    core, yy = lax.rem(t, 2), t // 2
    sib = yy * 2 + 1 - core
    far = (1 - yy) * 2
    zp = z + 1 - 2 * lax.rem(z, 2)
    middle = lax.rem((z + 1) // 2, 2)
    n_local = rows // LOCAL

    def aligned(v, m=ch):
        return pl.multiple_of(v, m)

    def y_row(zz, k):
        mid = lax.rem((zz + 1) // 2, 2)
        early = 1 - jnp.minimum(k // NE, 1)
        return (mid * NU + k + mid * lax.rem(zz, 2) * early * (NV - NE)) * ch

    def e_row(j):
        return (NU + (z // 2) * (NV - NE) + j) * ch

    def y_send_to(k, r):
        row = y_row(z, k)
        return pltpu.make_async_remote_copy(
            src_ref=a.at[pl.ds(aligned((far + r) * rows + row), ch)], dst_ref=arem.at[pl.ds(aligned(core * rows + row), ch)],
            send_sem=y_send, recv_sem=y_recv.at[core, k], device_id=(x, z, far + r), device_id_type=MESH)

    def start_y(k):
        for r in range(2):
            y_send_to(k, r).start()

    def move(row, s, recv, k, send, dev):
        ref = arem.at[pl.ds(aligned(s * rows + row), ch)]
        return pltpu.make_async_remote_copy(src_ref=ref, dst_ref=ref, send_sem=send, recv_sem=recv.at[s, k], device_id=dev, device_id_type=MESH)

    def each(row, recv, k, send, dev, start):
        for s in range(2):
            c = move(row, s, recv, k, send, dev)
            c.start() if start else c.wait_recv()

    def wait_y(k):
        each(y_row(z, k), y_recv, k, z_send, (x, zp, t), False)

    def relay_z(k):
        each(y_row(z, k), z_recv, k, z_send, (x, zp, t), True)

    def wait_z(k):
        each(y_row(zp, k), z_recv, k, z_send, (x, zp, t), False)

    def w_move(slot, part, idx, dev, src=None):
        ref = wbuf.at[pl.ds(aligned(slot * depth + part * half, 128), half)]
        return pltpu.make_async_remote_copy(src_ref=ref if src is None else src, dst_ref=ref, send_sem=w_send.at[idx], recv_sem=w_recv.at[idx],
                                            device_id=dev, device_id_type=MESH)

    w_sib = pltpu.make_async_remote_copy(src_ref=w, dst_ref=wbuf.at[pl.ds(depth, depth)], send_sem=w_send.at[0], recv_sem=w_recv.at[0],
                                         device_id=(x, z, sib), device_id_type=MESH)
    w_y = w_move(2 + core, x, 1, (x, z, far + core), w.at[pl.ds(aligned(x * half, 128), half)])
    w_x = w_move(2 + core, x, 2, (1 - x, z, t))
    w_x_in = w_move(2 + core, 1 - x, 2, (1 - x, z, t))
    w_d0 = w_move(2 + core, x, 3, (x, z, sib))
    w_d1 = w_move(2 + core, 1 - x, 4, (x, z, sib))
    w_d0_in = w_move(3 - core, x, 3, (x, z, sib))
    w_d1_in = w_move(3 - core, 1 - x, 4, (x, z, sib))

    def sib_copy(i):
        return pltpu.make_async_remote_copy(
            src_ref=a.at[pl.ds(aligned(sib * rows + i * LOCAL), LOCAL)], dst_ref=asib.at[pl.ds(aligned(i * LOCAL), LOCAL)],
            send_sem=sib_send, recv_sem=sib_recv.at[i], device_id=(x, z, sib), device_id_type=MESH)

    def loads(i):
        slot = lax.rem(i, 2)
        here = pl.ds(aligned(i * LOCAL), LOCAL)
        return (pltpu.make_async_copy(a.at[pl.ds(aligned(t * rows + i * LOCAL), LOCAL)], abuf.at[slot], ld.at[slot, 0]),
                pltpu.make_async_copy(asib.at[here], sbuf.at[slot], ld.at[slot, 1]),
                pltpu.make_async_copy(res.at[here], rbuf.at[slot], ld.at[slot, 2]))

    def prefetch(i):
        sib_copy(i).wait_recv()
        for c in loads(i):
            c.start()

    def block(lhs, slot, cols):
        return jnp.dot(lhs, wbuf[pl.ds(slot * depth, depth), cols], preferred_element_type=F32).astype(BF16).astype(F32)

    def local_tile(i):
        slot = lax.rem(i, 2)
        for c in loads(i):
            c.wait()

        @pl.when(i + 1 < n_local)
        def _():
            prefetch(i + 1)

        here = pl.ds(aligned(i * LOCAL), LOCAL)
        for n in range(width // 256):
            cols = pl.ds(n * 256, 256)
            h[here, cols] = rbuf[slot, :, cols].astype(F32) + block(abuf[slot], 0, cols) + block(sbuf[slot], 1, cols)

    def remote_tile(row):
        acc = jnp.zeros((TILE, 128), F32)
        here = pl.ds(aligned(row, TILE), TILE)
        there = pl.ds(aligned(rows + row, TILE), TILE)
        for n in range(width // 256):
            cols = pl.ds(n * 256, 256)
            v = h[here, cols] + block(arem[here, :], 2, cols) + block(arem[there, :], 3, cols)
            h[here, cols] = v
            sq = v * v
            acc = acc + sq[:, :128] + sq[:, 128:]
        ss_own[pl.ds(row // TILE, 1), :] = jnp.sum(acc.T, axis=0, keepdims=True)

    def pair(i):
        wait_z(2 * i)
        wait_z(2 * i + 1)

        def one(q, c):
            remote_tile(y_row(z + q * (zp - z), 2 * i))
            return c

        lax.fori_loop(0, 2, one, 0)

    for k in range(LOOK):
        start_y(k)
    own = pltpu.make_async_copy(w, wbuf.at[pl.ds(0, depth)], own_w)
    own.start()
    w_sib.start()
    lax.fori_loop(0, n_local, lambda i, c: (sib_copy(i).start(), c)[1], 0)
    prefetch(0)
    own.wait()
    w_sib.wait_recv()

    def first(k, c):
        wait_y(k)
        relay_z(k)

        @pl.when(middle == 1)
        def _():
            each(y_row(z, k), e_recv, k, e_send, (x, 3 - z, t), True)

        start_y(k + LOOK)

        @pl.when(k == 0)
        def _():
            w_y.start()

        local_tile(k)
        return c

    lax.fori_loop(0, NE, first, 0)

    def extra(j, c):
        local_tile(NE + 2 * j)
        each(e_row(j), e_recv, j, e_send, (x, zp, t), False)

        @pl.when(middle == 1)
        def _():
            each(e_row(j), e_recv, j, e_send, (x, zp, t), True)

        local_tile(NE + 2 * j + 1)
        return c

    lax.fori_loop(0, NE, extra, 0)
    w_y.wait_recv()
    w_x.start()
    w_d0.start()

    def second(k, c):
        wait_y(k)
        relay_z(k)
        start_y(k + LOOK)

        @pl.when(k < NE + 4)
        def _():
            local_tile(3 * NE + k - NE)

        return c

    lax.fori_loop(NE, 10, second, 0)
    w_x_in.wait_recv()
    w_d1.start()
    w_d0_in.wait_recv()
    w_d1_in.wait_recv()

    def step(k):
        wait_y(k)
        relay_z(k)

        @pl.when(k + LOOK < NY)
        def _():
            start_y(k + LOOK)

    def third(k, c):
        step(k)

        @pl.when(k == 10)
        def _():
            lax.fori_loop(0, 2, lambda j, d: (remote_tile(e_row(2 * j)), d)[1], 0)

        pair(k - 10)
        return c

    lax.fori_loop(10, 19, third, 0)

    def fourth(i, c):
        step(2 * i + 1)

        @pl.when(i < NY // 2 - 1)
        def _():
            step(2 * i + 2)

        pair(i)
        return c

    lax.fori_loop(9, NY // 2, fourth, 0)

    sends = []
    for d in range(1, 4):
        zz = lax.rem(z + d, 4)
        c = pltpu.make_async_remote_copy(src_ref=ss_own, dst_ref=ss_all.at[z], send_sem=ss_send.at[d], recv_sem=ss_recv.at[z],
                                         device_id=(x, zz, t), device_id_type=MESH)
        c.start()
        sends.append(c)
    y_total = 2 * NY * ch
    pltpu.make_async_remote_copy(src_ref=a.at[pl.ds(0, y_total)], dst_ref=arem.at[pl.ds(0, y_total)], send_sem=y_send, recv_sem=y_recv.at[0, 0],
                                 device_id=(x, z, far), device_id_type=MESH).wait_send()
    pltpu.make_async_remote_copy(src_ref=arem.at[pl.ds(0, y_total)], dst_ref=arem.at[pl.ds(0, y_total)], send_sem=z_send, recv_sem=z_recv.at[0, 0],
                                 device_id=(x, zp, t), device_id_type=MESH).wait_send()

    @pl.when(middle == 1)
    def _():
        n = 4 * NE * ch
        pltpu.make_async_remote_copy(src_ref=arem.at[pl.ds(0, n)], dst_ref=arem.at[pl.ds(0, n)], send_sem=e_send, recv_sem=e_recv.at[0, 0],
                                     device_id=(x, zp, t), device_id_type=MESH).wait_send()

    pltpu.make_async_remote_copy(src_ref=a.at[pl.ds(0, rows)], dst_ref=asib, send_sem=sib_send, recv_sem=sib_recv.at[0],
                                 device_id=(x, z, sib), device_id_type=MESH).wait_send()
    for c in (w_sib, w_y, w_x, w_d0, w_d1):
        c.wait_send()
    total = ss_own[...]
    for d in range(1, 4):
        zz = lax.rem(z + d, 4)
        pltpu.make_async_remote_copy(src_ref=ss_own, dst_ref=ss_all.at[zz], send_sem=ss_send.at[d], recv_sem=ss_recv.at[zz],
                                     device_id=(x, zz, t), device_id_type=MESH).wait_recv()
    ss_all[pl.ds(z, 1)] = total[None]
    ss_out[...] = (ss_all[0] + ss_all[1]) + (ss_all[2] + ss_all[3])
    for c in sends:
        c.wait_send()


def normalize(total_cols, h, ss, gain, h_out, n_out):
    i = pl.program_id(0)
    rows = h_out.shape[0]
    for b in range(rows // TILE):
        at = pl.multiple_of(i * rows + b * TILE, TILE)
        inv = lax.rsqrt(ss[pl.ds(i * (rows // TILE) + b, 1), :] / total_cols + EPS_NORM)
        inv = jnp.broadcast_to(inv, (TILE, TILE)).T
        here = pl.ds(b * TILE, TILE)
        for c in range(h_out.shape[1] // 128):
            cols = pl.ds(c * 128, 128)
            v = h[pl.ds(at, TILE), cols]
            h_out[here, cols] = v.astype(BF16)
            n_out[here, cols] = (v * inv * gain[:, cols]).astype(BF16)


def solution(mesh):
    col_groups = mesh.shape["tp2"]
    n_tp = mesh.shape["tp"]

    def local_step(a, w, res, gain):
        rows, width = res.shape
        depth = w.shape[0]
        dma = pltpu.SemaphoreType.DMA
        h, ss, _ = pl.pallas_call(
            gather_matmul,
            out_shape=(pltpu.VMEM((rows, width), F32), pltpu.VMEM((rows // TILE, 128), F32),
                       jax.ShapeDtypeStruct((rows, depth), BF16)),
            in_specs=[pl.BlockSpec(memory_space=pl.ANY)] * 3,
            out_specs=(pl.BlockSpec(memory_space=pltpu.VMEM), pl.BlockSpec(memory_space=pltpu.VMEM), pl.BlockSpec(memory_space=pl.ANY)),
            scratch_shapes=[
                pltpu.VMEM((2 * rows, depth), BF16), pltpu.VMEM((n_tp * depth, width), BF16),
                pltpu.VMEM((2, LOCAL, depth), BF16), pltpu.VMEM((2, LOCAL, depth), BF16), pltpu.VMEM((2, LOCAL, width), BF16),
                pltpu.VMEM((rows // TILE, 128), F32), pltpu.VMEM((4, rows // TILE, 128), F32),
                dma((2, 3)), dma, dma((rows // LOCAL,)), dma, dma((2, NY)), dma, dma((2, NY)), dma, dma((2, NE)), dma,
                dma((5,)), dma((5,)), dma((4,)), dma((4,)),
            ],
            compiler_params=pltpu.CompilerParams(has_side_effects=True, vmem_limit_bytes=42 * 1024 * 1024),
            cost_estimate=pl.CostEstimate(flops=2 * rows * n_tp * depth * width, bytes_accessed=8 * rows * width, transcendentals=0),
            name="gather_matmul",
        )(a, w, res)
        blk = 512
        return pl.pallas_call(
            functools.partial(normalize, width * col_groups),
            grid=(rows // blk,),
            out_shape=(jax.ShapeDtypeStruct((rows, width), BF16),) * 2,
            in_specs=[pl.BlockSpec(memory_space=pltpu.VMEM)] * 3,
            out_specs=(pl.BlockSpec((blk, width), lambda i: (i, 0)),) * 2,
            compiler_params=pltpu.CompilerParams(vmem_limit_bytes=16 * 1024 * 1024),
            name="normalize",
        )(h, ss, gain.reshape(1, width))

    row_spec = P(("dp", "tp"), "tp2")
    return jax.shard_map(local_step, mesh=mesh, in_specs=(P("dp", "tp"), P("tp", "tp2"), row_spec, P("tp2")), out_specs=(row_spec, row_spec), check_vma=False)
```

```python
import functools

import jax
import jax.numpy as jnp
from jax import lax
from jax.experimental import pallas as pl
from jax.experimental.pallas import tpu as pltpu
from jax.sharding import PartitionSpec as P

EPS_NORM = 1e-6
MESH = pl.DeviceIdType.MESH
F32, BF16 = jnp.float32, jnp.bfloat16

NCH, NU, NY, NR, NE = 128, 60, 60, 56, 12
LOOK = 6
CATCH, CAUGHT = 24, 10
TILE = 128
LOCAL = 256
STORE = 128


def gather_matmul(a, w, res, h, ss_out, asib, arem, wbuf, abuf, sbuf, rbuf, ss_own, ss_all,
                  ss_last, ss_lasts, ld, own_w, sib_recv, sib_send, y_recv, y_send, z_recv, z_send, e_recv, e_send, w_recv, w_send, ss_recv, ss_send, sl_recv, sl_send):
    x, z, t = lax.axis_index("dp"), lax.axis_index("tp2"), lax.axis_index("tp")
    rows, width = h.shape
    depth = w.shape[0]
    half = depth // 2
    ch = rows // NCH
    core, yy = lax.rem(t, 2), t // 2
    sib = yy * 2 + 1 - core
    far = (1 - yy) * 2
    zp = z + 1 - 2 * lax.rem(z, 2)
    middle = lax.rem((z + 1) // 2, 2)
    n_local = rows // LOCAL

    def aligned(v, m=ch):
        return pl.multiple_of(v, m)

    def y_row(zz, k):
        mid = lax.rem((zz + 1) // 2, 2)
        early = 1 - jnp.minimum(k // NE, 1)
        late = jnp.minimum(k // NR, 1)
        return (k + mid * (1 - late) * NU + mid * lax.rem(zz, 2) * early * NR) * ch

    def e_row(j):
        return (NU + (z // 2) * NR + j) * ch

    def y_send_to(k, r):
        row = y_row(z, k)
        return pltpu.make_async_remote_copy(
            src_ref=a.at[pl.ds(aligned((far + r) * rows + row), ch)], dst_ref=arem.at[pl.ds(aligned(core * rows + row), ch)],
            send_sem=y_send, recv_sem=y_recv.at[core, k], device_id=(x, z, far + r), device_id_type=MESH)

    def start_y(k):
        for r in range(2):
            y_send_to(k, r).start()

    def move(row, s, recv, k, send, dev):
        ref = arem.at[pl.ds(aligned(s * rows + row), ch)]
        return pltpu.make_async_remote_copy(src_ref=ref, dst_ref=ref, send_sem=send, recv_sem=recv.at[s, k], device_id=dev, device_id_type=MESH)

    def each(row, recv, k, send, dev, start):
        for s in range(2):
            c = move(row, s, recv, k, send, dev)
            c.start() if start else c.wait_recv()

    def wait_y(k):
        each(y_row(z, k), y_recv, k, z_send, (x, zp, t), False)

    def relay_z(k):
        each(y_row(z, k), z_recv, k, z_send, (x, zp, t), True)

    def wait_z(k):
        each(y_row(zp, k), z_recv, k, z_send, (x, zp, t), False)

    def w_move(slot, part, idx, dev, src=None):
        ref = wbuf.at[pl.ds(aligned(slot * depth + part * half, 128), half)]
        return pltpu.make_async_remote_copy(src_ref=ref if src is None else src, dst_ref=ref, send_sem=w_send.at[idx], recv_sem=w_recv.at[idx],
                                            device_id=dev, device_id_type=MESH)

    w_sib = pltpu.make_async_remote_copy(src_ref=w, dst_ref=wbuf.at[pl.ds(depth, depth)], send_sem=w_send.at[0], recv_sem=w_recv.at[0],
                                         device_id=(x, z, sib), device_id_type=MESH)
    w_y = w_move(2 + core, x, 1, (x, z, far + core), w.at[pl.ds(aligned(x * half, 128), half)])
    w_x = w_move(2 + core, x, 2, (1 - x, z, t))
    w_x_in = w_move(2 + core, 1 - x, 2, (1 - x, z, t))
    w_d0 = w_move(2 + core, x, 3, (x, z, sib))
    w_d1 = w_move(2 + core, 1 - x, 4, (x, z, sib))
    w_d0_in = w_move(3 - core, x, 3, (x, z, sib))
    w_d1_in = w_move(3 - core, 1 - x, 4, (x, z, sib))

    def sib_copy(i):
        return pltpu.make_async_remote_copy(
            src_ref=a.at[pl.ds(aligned(sib * rows + i * LOCAL), LOCAL)], dst_ref=asib.at[pl.ds(aligned(i * LOCAL), LOCAL)],
            send_sem=sib_send, recv_sem=sib_recv.at[i], device_id=(x, z, sib), device_id_type=MESH)

    def loads(i):
        slot = lax.rem(i, 2)
        here = pl.ds(aligned(i * LOCAL), LOCAL)
        return (pltpu.make_async_copy(a.at[pl.ds(aligned(t * rows + i * LOCAL), LOCAL)], abuf.at[slot], ld.at[slot, 0]),
                pltpu.make_async_copy(asib.at[here], sbuf.at[slot], ld.at[slot, 1]),
                pltpu.make_async_copy(res.at[here], rbuf.at[slot], ld.at[slot, 2]))

    def prefetch(i):
        sib_copy(i).wait_recv()
        for c in loads(i):
            c.start()

    def block(lhs, slot, cols):
        return jnp.dot(lhs, wbuf[pl.ds(slot * depth, depth), cols], preferred_element_type=F32).astype(BF16).astype(F32)

    def local_tile(i):
        slot = lax.rem(i, 2)
        for c in loads(i):
            c.wait()

        @pl.when(i + 1 < n_local)
        def _():
            prefetch(i + 1)

        here = pl.ds(aligned(i * LOCAL), LOCAL)
        for n in range(width // 256):
            cols = pl.ds(n * 256, 256)
            h[here, cols] = rbuf[slot, :, cols].astype(F32) + block(abuf[slot], 0, cols) + block(sbuf[slot], 1, cols)

    def remote_tile(row):
        acc = jnp.zeros((TILE, 128), F32)
        here = pl.ds(aligned(row, TILE), TILE)
        there = pl.ds(aligned(rows + row, TILE), TILE)
        for n in range(width // 256):
            cols = pl.ds(n * 256, 256)
            v = h[here, cols] + block(arem[here, :], 2, cols) + block(arem[there, :], 3, cols)
            h[here, cols] = v
            sq = v * v
            acc = acc + sq[:, :128] + sq[:, 128:]
        return jnp.sum(acc.T, axis=0, keepdims=True)

    def tile(row):
        ss_own[pl.ds(row // TILE, 1), :] = remote_tile(row)

    cpt = TILE // ch

    def y_tile(i):
        tile(y_row(z, cpt * i))

    def z_tile(i):
        for s in range(cpt):
            wait_z(cpt * i + s)
        tile(y_row(zp, cpt * i))

    barrier = pltpu.get_barrier_semaphore()
    partners = [(x, z, far), (x, z, far + 1), (x, z, sib), (1 - x, z, t)] + [(x, lax.rem(z + d, 4), t) for d in range(1, 4)]
    for dev in partners:
        pl.semaphore_signal(barrier, inc=1, device_id=dev, device_id_type=MESH)
    pl.semaphore_wait(barrier, len(partners))

    for k in range(LOOK):
        start_y(k)
    own = pltpu.make_async_copy(w, wbuf.at[pl.ds(0, depth)], own_w)
    own.start()
    w_sib.start()
    lax.fori_loop(0, n_local, lambda i, c: (sib_copy(i).start(), c)[1], 0)
    prefetch(0)
    own.wait()
    w_sib.wait_recv()

    def step(k):
        wait_y(k)

        @pl.when(k < NR)
        def _():
            relay_z(k)

        @pl.when(k + LOOK < NY)
        def _():
            start_y(k + LOOK)

    def first(k, c):
        step(k)

        @pl.when(middle == 1)
        def _():
            each(y_row(z, k), e_recv, k, e_send, (x, 3 - z, t), True)

        @pl.when(k == NE - 1 - LOOK)
        def _():
            w_y.start()

        @pl.when(lax.rem(k, 2) == 1)
        def _():
            local_tile(k // 2)

        return c

    lax.fori_loop(0, NE, first, 0)

    def extra(j, c):
        each(e_row(j), e_recv, j, e_send, (x, zp, t), False)

        @pl.when(middle == 1)
        def _():
            each(e_row(j), e_recv, j, e_send, (x, zp, t), True)

        @pl.when(NE // 2 + j < n_local)
        def _():
            local_tile(NE // 2 + j)

        return c

    lax.fori_loop(0, NE, extra, 0)
    w_y.wait_recv()
    w_x.start()
    w_d0.start()
    lax.fori_loop(NE, CATCH, lambda k, c: (step(k), c)[1], 0)
    w_x_in.wait_recv()
    w_d1.start()
    w_d0_in.wait_recv()
    w_d1_in.wait_recv()

    def third(i, c):
        step(CATCH + 2 * i)

        @pl.when(i == 0)
        def _():
            lax.fori_loop(0, NE // cpt, lambda j, d: (tile(e_row(cpt * j)), d)[1], 0)

        y_tile(i)
        step(CATCH + 2 * i + 1)
        z_tile(i)
        return c

    lax.fori_loop(0, CAUGHT, third, 0)

    def steps(lo, hi):
        lax.fori_loop(jnp.maximum(lo, CATCH + 2 * CAUGHT), jnp.minimum(hi, NY), lambda k, c: (step(k), c)[1], 0)

    def fourth(i, c):
        steps(cpt * i + 1, cpt * i + cpt)
        y_tile(i)
        steps(cpt * i + cpt, cpt * i + cpt + 1)
        z_tile(i)
        return c

    lax.fori_loop(CAUGHT, NR // cpt, fourth, 0)
    steps(NR + 1, NY)

    def share(src, dst, send, recv):
        for d in range(1, 4):
            pltpu.make_async_remote_copy(src_ref=src, dst_ref=dst.at[z], send_sem=send.at[d], recv_sem=recv.at[z],
                                         device_id=(x, lax.rem(z + d, 4), t), device_id_type=MESH).start()

    def collect(src, dst, send, recv):
        for d in range(1, 4):
            zz = lax.rem(z + d, 4)
            pltpu.make_async_remote_copy(src_ref=src, dst_ref=dst.at[zz], send_sem=send.at[d], recv_sem=recv.at[zz],
                                         device_id=(x, zz, t), device_id_type=MESH).wait()
        dst[pl.ds(z, 1)] = src[...][None]
        return (dst[0] + dst[1]) + (dst[2] + dst[3])

    share(ss_own, ss_all, ss_send, ss_recv)
    ss_last[...] = jnp.broadcast_to(remote_tile(NR * ch), ss_last.shape)
    share(ss_last, ss_lasts, sl_send, sl_recv)
    y_total = 2 * NY * ch
    pltpu.make_async_remote_copy(src_ref=a.at[pl.ds(0, y_total)], dst_ref=arem.at[pl.ds(0, y_total)], send_sem=y_send, recv_sem=y_recv.at[0, 0],
                                 device_id=(x, z, far), device_id_type=MESH).wait_send()
    z_total = 2 * NR * ch
    pltpu.make_async_remote_copy(src_ref=arem.at[pl.ds(0, z_total)], dst_ref=arem.at[pl.ds(0, z_total)], send_sem=z_send, recv_sem=z_recv.at[0, 0],
                                 device_id=(x, zp, t), device_id_type=MESH).wait_send()

    @pl.when(middle == 1)
    def _():
        n = 4 * NE * ch
        pltpu.make_async_remote_copy(src_ref=arem.at[pl.ds(0, n)], dst_ref=arem.at[pl.ds(0, n)], send_sem=e_send, recv_sem=e_recv.at[0, 0],
                                     device_id=(x, zp, t), device_id_type=MESH).wait_send()

    pltpu.make_async_remote_copy(src_ref=a.at[pl.ds(0, rows)], dst_ref=asib, send_sem=sib_send, recv_sem=sib_recv.at[0],
                                 device_id=(x, z, sib), device_id_type=MESH).wait_send()
    for c in (w_sib, w_y, w_x, w_d0, w_d1):
        c.wait_send()
    ss_out[...] = collect(ss_own, ss_all, ss_send, ss_recv)
    ss_out[pl.ds(NR * ch // TILE, 1), :] = collect(ss_last, ss_lasts, sl_send, sl_recv)[:1]


def normalize(total_cols, h, ss, gain, h_hbm, n_hbm, h_out, n_out, sem):
    n_blocks = h.shape[0] // STORE

    def out(i):
        here = pl.ds(pl.multiple_of(i * STORE, STORE), STORE)
        buf = pl.ds(pl.multiple_of(lax.rem(i, n_blocks // 2) * STORE, STORE), STORE)
        return (pltpu.make_async_copy(h_out.at[buf], h_hbm.at[here], sem.at[0, i]),
                pltpu.make_async_copy(n_out.at[buf], n_hbm.at[here], sem.at[1, i]))

    def start(i):
        for c in out(i):
            c.start()

    def wait(i):
        for c in out(i):
            c.wait()

    def block(i, carry):
        @pl.when(i >= n_blocks // 2)
        def _():
            wait(i - n_blocks // 2)

        for b in range(STORE // TILE):
            here = pl.ds(pl.multiple_of(i * STORE + b * TILE, TILE), TILE)
            to = pl.ds(pl.multiple_of(lax.rem(i, n_blocks // 2) * STORE + b * TILE, TILE), TILE)
            inv = lax.rsqrt(ss[pl.ds(i * (STORE // TILE) + b, 1), :] / total_cols + EPS_NORM)
            inv = jnp.broadcast_to(inv, (TILE, TILE)).T
            for c in range(h.shape[1] // 128):
                cols = pl.ds(c * 128, 128)
                v = h[here, cols]
                h_out[to, cols] = v.astype(BF16)
                n_out[to, cols] = (v * inv * gain[cols][None, :]).astype(BF16)

        @pl.when(i > 0)
        def _():
            start(i - 1)

        return carry

    lax.fori_loop(0, n_blocks, block, 0)
    start(n_blocks - 1)
    lax.fori_loop(n_blocks // 2, n_blocks, lambda i, c: (wait(i), c)[1], 0)


def solution(mesh):
    col_groups = mesh.shape["tp2"]
    n_tp = mesh.shape["tp"]

    def local_step(a, w, res, gain):
        rows, width = res.shape
        depth = w.shape[0]
        dma = pltpu.SemaphoreType.DMA
        h, ss, _ = pl.pallas_call(
            gather_matmul,
            out_shape=(pltpu.VMEM((rows, width), F32), pltpu.VMEM((rows // TILE, 128), F32),
                       jax.ShapeDtypeStruct((rows, depth), BF16)),
            in_specs=[pl.BlockSpec(memory_space=pl.ANY)] * 3,
            out_specs=(pl.BlockSpec(memory_space=pltpu.VMEM), pl.BlockSpec(memory_space=pltpu.VMEM), pl.BlockSpec(memory_space=pl.ANY)),
            scratch_shapes=[
                pltpu.VMEM((2 * rows, depth), BF16), pltpu.VMEM((n_tp * depth, width), BF16),
                pltpu.VMEM((2, LOCAL, depth), BF16), pltpu.VMEM((2, LOCAL, depth), BF16), pltpu.VMEM((2, LOCAL, width), BF16),
                pltpu.VMEM((rows // TILE, 128), F32), pltpu.VMEM((4, rows // TILE, 128), F32), pltpu.VMEM((8, 128), F32), pltpu.VMEM((4, 8, 128), F32),
                dma((2, 3)), dma, dma((rows // LOCAL,)), dma, dma((2, NY)), dma, dma((2, NY)), dma, dma((2, NE)), dma,
                dma((5,)), dma((5,)), dma((4,)), dma((4,)), dma((4,)), dma((4,)),
            ],
            compiler_params=pltpu.CompilerParams(collective_id=0, has_side_effects=True, vmem_limit_bytes=42 * 1024 * 1024),
            cost_estimate=pl.CostEstimate(flops=2 * rows * n_tp * depth * width, bytes_accessed=8 * rows * width, transcendentals=0),
            name="gather_matmul",
        )(a, w, res)
        return pl.pallas_call(
            functools.partial(normalize, width * col_groups),
            out_shape=(jax.ShapeDtypeStruct((rows, width), BF16),) * 2,
            in_specs=[pl.BlockSpec(memory_space=pltpu.VMEM)] * 3,
            out_specs=(pl.BlockSpec(memory_space=pl.ANY),) * 2,
            scratch_shapes=[pltpu.VMEM((rows // 2, width), BF16), pltpu.VMEM((rows // 2, width), BF16), dma((2, rows // STORE))],
            compiler_params=pltpu.CompilerParams(vmem_limit_bytes=14 * 1024 * 1024),
            name="normalize",
        )(h, ss, gain)

    row_spec = P(("dp", "tp"), "tp2")
    return jax.shard_map(local_step, mesh=mesh, in_specs=(P("dp", "tp"), P("tp", "tp2"), row_spec, P("tp2")), out_specs=(row_spec, row_spec), check_vma=False)
```

```python
import functools

import jax
import jax.numpy as jnp
from jax import lax
from jax.experimental import pallas as pl
from jax.experimental.pallas import tpu as pltpu
from jax.sharding import PartitionSpec as P

EPS_NORM = 1e-6
MESH = pl.DeviceIdType.MESH
F32, BF16 = jnp.float32, jnp.bfloat16

SPLIT = 1
NCH, NU, NY, NR, NE = 128 * SPLIT, 60 * SPLIT, 60 * SPLIT, 56 * SPLIT, 12 * SPLIT
LOOK, LAG = 6 * SPLIT, 3
CATCH, CAUGHT = 24 * SPLIT, 10
TILE = 128
LOCAL = 256
STORE = 128


def gather_matmul(a, w, res, h, ss_out, asib, arem, wbuf, abuf, sbuf, rbuf, ss_own, ss_all,
                  ss_last, ss_lasts, ld, own_w, sib_recv, sib_send, y_recv, y_send, z_recv, z_send, e_recv, e_send, w_recv, w_send, ss_recv, ss_send, sl_recv, sl_send):
    x, z, t = lax.axis_index("dp"), lax.axis_index("tp2"), lax.axis_index("tp")
    rows, width = h.shape
    depth = w.shape[0]
    half = depth // 2
    ch = rows // NCH
    core, yy = lax.rem(t, 2), t // 2
    sib = yy * 2 + 1 - core
    far = (1 - yy) * 2
    zp = z + 1 - 2 * lax.rem(z, 2)
    middle = lax.rem((z + 1) // 2, 2)
    n_local = rows // LOCAL

    def aligned(v, m=ch):
        return pl.multiple_of(v, m)

    def y_row(zz, k):
        mid = lax.rem((zz + 1) // 2, 2)
        early = 1 - jnp.minimum(k // NE, 1)
        late = jnp.minimum(k // NR, 1)
        return (k + mid * (1 - late) * NU + mid * lax.rem(zz, 2) * early * NR) * ch

    def e_row(j):
        return (NU + (z // 2) * NR + j) * ch

    def y_send_to(k, r):
        row = y_row(z, k)
        return pltpu.make_async_remote_copy(
            src_ref=a.at[pl.ds(aligned((far + r) * rows + row), ch)], dst_ref=arem.at[pl.ds(aligned(core * rows + row), ch)],
            send_sem=y_send, recv_sem=y_recv.at[core, k], device_id=(x, z, far + r), device_id_type=MESH)

    def start_y(k):
        for r in range(2):
            y_send_to(k, r).start()

    def move(row, s, recv, k, send, dev):
        ref = arem.at[pl.ds(aligned(s * rows + row), ch)]
        return pltpu.make_async_remote_copy(src_ref=ref, dst_ref=ref, send_sem=send, recv_sem=recv.at[s, k], device_id=dev, device_id_type=MESH)

    def each(row, recv, k, send, dev, start):
        for s in range(2):
            c = move(row, s, recv, k, send, dev)
            c.start() if start else c.wait_recv()

    def wait_y(k):
        each(y_row(z, k), y_recv, k, z_send, (x, zp, t), False)

    def relay_z(k):
        each(y_row(z, k), z_recv, k, z_send, (x, zp, t), True)

    def wait_z(k):
        each(y_row(zp, k), z_recv, k, z_send, (x, zp, t), False)

    def w_move(slot, part, idx, dev, src=None):
        ref = wbuf.at[pl.ds(aligned(slot * depth + part * half, 128), half)]
        return pltpu.make_async_remote_copy(src_ref=ref if src is None else src, dst_ref=ref, send_sem=w_send.at[idx], recv_sem=w_recv.at[idx],
                                            device_id=dev, device_id_type=MESH)

    w_sib = pltpu.make_async_remote_copy(src_ref=w, dst_ref=wbuf.at[pl.ds(depth, depth)], send_sem=w_send.at[0], recv_sem=w_recv.at[0],
                                         device_id=(x, z, sib), device_id_type=MESH)
    w_y = w_move(2 + core, x, 1, (x, z, far + core), w.at[pl.ds(aligned(x * half, 128), half)])
    w_x = w_move(2 + core, x, 2, (1 - x, z, t))
    w_x_in = w_move(2 + core, 1 - x, 2, (1 - x, z, t))
    w_d0 = w_move(2 + core, x, 3, (x, z, sib))
    w_d1 = w_move(2 + core, 1 - x, 4, (x, z, sib))
    w_d0_in = w_move(3 - core, x, 3, (x, z, sib))
    w_d1_in = w_move(3 - core, 1 - x, 4, (x, z, sib))

    def sib_copy(i):
        return pltpu.make_async_remote_copy(
            src_ref=a.at[pl.ds(aligned(sib * rows + i * LOCAL), LOCAL)], dst_ref=asib.at[pl.ds(aligned(i * LOCAL), LOCAL)],
            send_sem=sib_send, recv_sem=sib_recv.at[i], device_id=(x, z, sib), device_id_type=MESH)

    def loads(i):
        slot = lax.rem(i, 2)
        here = pl.ds(aligned(i * LOCAL), LOCAL)
        return (pltpu.make_async_copy(a.at[pl.ds(aligned(t * rows + i * LOCAL), LOCAL)], abuf.at[slot], ld.at[slot, 0]),
                pltpu.make_async_copy(asib.at[here], sbuf.at[slot], ld.at[slot, 1]),
                pltpu.make_async_copy(res.at[here], rbuf.at[slot], ld.at[slot, 2]))

    def prefetch(i):
        sib_copy(i).wait_recv()
        for c in loads(i):
            c.start()

    def block(lhs, slot, cols):
        return jnp.dot(lhs, wbuf[pl.ds(slot * depth, depth), cols], preferred_element_type=F32).astype(BF16).astype(F32)

    def local_tile(i):
        slot = lax.rem(i, 2)
        for c in loads(i):
            c.wait()

        @pl.when(i + 1 < n_local)
        def _():
            prefetch(i + 1)

        here = pl.ds(aligned(i * LOCAL), LOCAL)
        for n in range(width // 256):
            cols = pl.ds(n * 256, 256)
            h[here, cols] = rbuf[slot, :, cols].astype(F32) + block(abuf[slot], 0, cols) + block(sbuf[slot], 1, cols)

    def remote_tile(row):
        acc = jnp.zeros((TILE, 128), F32)
        here = pl.ds(aligned(row, TILE), TILE)
        there = pl.ds(aligned(rows + row, TILE), TILE)
        for n in range(width // 256):
            cols = pl.ds(n * 256, 256)
            v = h[here, cols] + block(arem[here, :], 2, cols) + block(arem[there, :], 3, cols)
            h[here, cols] = v
            sq = v * v
            acc = acc + sq[:, :128] + sq[:, 128:]
        return jnp.sum(acc.T, axis=0, keepdims=True)

    def tile(row):
        ss_own[pl.ds(row // TILE, 1), :] = remote_tile(row)

    cpt = TILE // ch

    def y_tile(i):
        tile(y_row(z, cpt * i))

    def z_tile(i):
        for s in range(cpt):
            wait_z(cpt * i + s)
        tile(y_row(zp, cpt * i))

    barrier = pltpu.get_barrier_semaphore()
    partners = [(x, z, far), (x, z, far + 1), (x, z, sib), (1 - x, z, t)] + [(x, lax.rem(z + d, 4), t) for d in range(1, 4)]
    for dev in partners:
        pl.semaphore_signal(barrier, inc=1, device_id=dev, device_id_type=MESH)
    pl.semaphore_wait(barrier, len(partners))

    for k in range(LOOK):
        start_y(k)
    own = pltpu.make_async_copy(w, wbuf.at[pl.ds(0, depth)], own_w)
    own.start()
    w_sib.start()
    lax.fori_loop(0, n_local, lambda i, c: (sib_copy(i).start(), c)[1], 0)
    prefetch(0)
    own.wait()
    w_sib.wait_recv()

    def step(k):
        wait_y(k)

        @pl.when(k < NR)
        def _():
            relay_z(k)

        @pl.when(k + LOOK < NY)
        def _():
            start_y(k + LOOK)

    def first(k, c):
        step(k)

        @pl.when(middle == 1)
        def _():
            each(y_row(z, k), e_recv, k, e_send, (x, 3 - z, t), True)

        @pl.when(k == NE - 1 - LOOK)
        def _():
            w_y.start()

        @pl.when((middle == 1) & (k >= LAG))
        def _():
            swap(k - LAG)

        @pl.when(lax.rem(k, 2 * SPLIT) == 2 * SPLIT - 1)
        def _():
            local_tile(k // (2 * SPLIT))

        return c

    def extra(j):
        each(e_row(j), e_recv, j, e_send, (x, zp, t), False)

    def swap(j):
        extra(j)
        each(e_row(j), e_recv, j, e_send, (x, zp, t), True)

    lax.fori_loop(0, NE, first, 0)
    lax.fori_loop(NE - middle * LAG, NE, lambda j, c: (swap(j), c)[1], 0)
    lax.fori_loop(NE // (2 * SPLIT), n_local, lambda i, c: (local_tile(i), c)[1], 0)
    w_y.wait_recv()
    w_x.start()
    w_d0.start()
    lax.fori_loop(NE, CATCH, lambda k, c: (step(k), c)[1], 0)
    w_x_in.wait_recv()
    w_d1.start()
    w_d0_in.wait_recv()
    w_d1_in.wait_recv()

    def third(i, c):
        for s in range(SPLIT):
            step(CATCH + 2 * SPLIT * i + s)

        @pl.when(i == 0)
        def _():
            lax.fori_loop(middle * NE, NE, lambda j, c: (extra(j), c)[1], 0)
            lax.fori_loop(0, NE // cpt, lambda j, d: (tile(e_row(cpt * j)), d)[1], 0)

        y_tile(i)
        for s in range(SPLIT):
            step(CATCH + 2 * SPLIT * i + SPLIT + s)

        @pl.when(i < CAUGHT - 1)
        def _():
            z_tile(i)

        return c

    lax.fori_loop(0, CAUGHT, third, 0)

    def steps(lo, hi):
        lax.fori_loop(jnp.maximum(lo, CATCH + 2 * SPLIT * CAUGHT), jnp.minimum(hi, NY), lambda k, c: (step(k), c)[1], 0)

    def fourth(i, c):
        steps(cpt * i + 1, cpt * i + cpt)
        y_tile(i)
        steps(cpt * i + cpt, cpt * i + cpt + 1)
        z_tile(i - 1)
        return c

    lax.fori_loop(CAUGHT, NR // cpt, fourth, 0)
    steps(NR + 1, NY - 1)
    z_tile(NR // cpt - 1)
    steps(NY - 1, NY)

    def share(src, dst, send, recv):
        for d in range(1, 4):
            pltpu.make_async_remote_copy(src_ref=src, dst_ref=dst.at[z], send_sem=send.at[d], recv_sem=recv.at[z],
                                         device_id=(x, lax.rem(z + d, 4), t), device_id_type=MESH).start()

    def collect(src, dst, send, recv):
        for d in range(1, 4):
            zz = lax.rem(z + d, 4)
            pltpu.make_async_remote_copy(src_ref=src, dst_ref=dst.at[zz], send_sem=send.at[d], recv_sem=recv.at[zz],
                                         device_id=(x, zz, t), device_id_type=MESH).wait()
        dst[pl.ds(z, 1)] = src[...][None]
        return (dst[0] + dst[1]) + (dst[2] + dst[3])

    share(ss_own, ss_all, ss_send, ss_recv)
    ss_last[...] = jnp.broadcast_to(remote_tile(NR * ch), ss_last.shape)
    share(ss_last, ss_lasts, sl_send, sl_recv)
    y_total = 2 * NY * ch
    pltpu.make_async_remote_copy(src_ref=a.at[pl.ds(0, y_total)], dst_ref=arem.at[pl.ds(0, y_total)], send_sem=y_send, recv_sem=y_recv.at[0, 0],
                                 device_id=(x, z, far), device_id_type=MESH).wait_send()
    z_total = 2 * NR * ch
    pltpu.make_async_remote_copy(src_ref=arem.at[pl.ds(0, z_total)], dst_ref=arem.at[pl.ds(0, z_total)], send_sem=z_send, recv_sem=z_recv.at[0, 0],
                                 device_id=(x, zp, t), device_id_type=MESH).wait_send()

    @pl.when(middle == 1)
    def _():
        n = 4 * NE * ch
        pltpu.make_async_remote_copy(src_ref=arem.at[pl.ds(0, n)], dst_ref=arem.at[pl.ds(0, n)], send_sem=e_send, recv_sem=e_recv.at[0, 0],
                                     device_id=(x, zp, t), device_id_type=MESH).wait_send()

    pltpu.make_async_remote_copy(src_ref=a.at[pl.ds(0, rows)], dst_ref=asib, send_sem=sib_send, recv_sem=sib_recv.at[0],
                                 device_id=(x, z, sib), device_id_type=MESH).wait_send()
    for c in (w_sib, w_y, w_x, w_d0, w_d1):
        c.wait_send()
    ss_out[...] = collect(ss_own, ss_all, ss_send, ss_recv)
    ss_out[pl.ds(NR * ch // TILE, 1), :] = collect(ss_last, ss_lasts, sl_send, sl_recv)[:1]


def normalize(total_cols, h, ss, gain, h_hbm, n_hbm, h_out, n_out, sem):
    n_blocks = h.shape[0] // STORE

    def out(i):
        here = pl.ds(pl.multiple_of(i * STORE, STORE), STORE)
        buf = pl.ds(pl.multiple_of(lax.rem(i, n_blocks // 2) * STORE, STORE), STORE)
        return (pltpu.make_async_copy(h_out.at[buf], h_hbm.at[here], sem.at[0, i]),
                pltpu.make_async_copy(n_out.at[buf], n_hbm.at[here], sem.at[1, i]))

    def start(i):
        for c in out(i):
            c.start()

    def wait(i):
        for c in out(i):
            c.wait()

    def block(i, carry):
        @pl.when(i >= n_blocks // 2)
        def _():
            wait(i - n_blocks // 2)

        for b in range(STORE // TILE):
            here = pl.ds(pl.multiple_of(i * STORE + b * TILE, TILE), TILE)
            to = pl.ds(pl.multiple_of(lax.rem(i, n_blocks // 2) * STORE + b * TILE, TILE), TILE)
            inv = lax.rsqrt(ss[pl.ds(i * (STORE // TILE) + b, 1), :] / total_cols + EPS_NORM)
            inv = jnp.broadcast_to(inv, (TILE, TILE)).T
            for c in range(h.shape[1] // 128):
                cols = pl.ds(c * 128, 128)
                v = h[here, cols]
                h_out[to, cols] = v.astype(BF16)
                n_out[to, cols] = (v * inv * gain[cols][None, :]).astype(BF16)

        @pl.when(i > 0)
        def _():
            start(i - 1)

        return carry

    lax.fori_loop(0, n_blocks, block, 0)
    start(n_blocks - 1)
    lax.fori_loop(n_blocks // 2, n_blocks, lambda i, c: (wait(i), c)[1], 0)


def solution(mesh):
    col_groups = mesh.shape["tp2"]
    n_tp = mesh.shape["tp"]

    def local_step(a, w, res, gain):
        rows, width = res.shape
        depth = w.shape[0]
        dma = pltpu.SemaphoreType.DMA
        h, ss, _ = pl.pallas_call(
            gather_matmul,
            out_shape=(pltpu.VMEM((rows, width), F32), pltpu.VMEM((rows // TILE, 128), F32),
                       jax.ShapeDtypeStruct((rows, depth), BF16)),
            in_specs=[pl.BlockSpec(memory_space=pl.ANY)] * 3,
            out_specs=(pl.BlockSpec(memory_space=pltpu.VMEM), pl.BlockSpec(memory_space=pltpu.VMEM), pl.BlockSpec(memory_space=pl.ANY)),
            scratch_shapes=[
                pltpu.VMEM((2 * rows, depth), BF16), pltpu.VMEM((n_tp * depth, width), BF16),
                pltpu.VMEM((2, LOCAL, depth), BF16), pltpu.VMEM((2, LOCAL, depth), BF16), pltpu.VMEM((2, LOCAL, width), BF16),
                pltpu.VMEM((rows // TILE, 128), F32), pltpu.VMEM((4, rows // TILE, 128), F32), pltpu.VMEM((8, 128), F32), pltpu.VMEM((4, 8, 128), F32),
                dma((2, 3)), dma, dma((rows // LOCAL,)), dma, dma((2, NY)), dma, dma((2, NY)), dma, dma((2, NE)), dma,
                dma((5,)), dma((5,)), dma((4,)), dma((4,)), dma((4,)), dma((4,)),
            ],
            compiler_params=pltpu.CompilerParams(collective_id=0, has_side_effects=True, vmem_limit_bytes=42 * 1024 * 1024),
            cost_estimate=pl.CostEstimate(flops=2 * rows * n_tp * depth * width, bytes_accessed=8 * rows * width, transcendentals=0),
            name="gather_matmul",
        )(a, w, res)
        return pl.pallas_call(
            functools.partial(normalize, width * col_groups),
            out_shape=(jax.ShapeDtypeStruct((rows, width), BF16),) * 2,
            in_specs=[pl.BlockSpec(memory_space=pltpu.VMEM)] * 3,
            out_specs=(pl.BlockSpec(memory_space=pl.ANY),) * 2,
            scratch_shapes=[pltpu.VMEM((rows // 2, width), BF16), pltpu.VMEM((rows // 2, width), BF16), dma((2, rows // STORE))],
            compiler_params=pltpu.CompilerParams(vmem_limit_bytes=14 * 1024 * 1024),
            name="normalize",
        )(h, ss, gain)

    row_spec = P(("dp", "tp"), "tp2")
    return jax.shard_map(local_step, mesh=mesh, in_specs=(P("dp", "tp"), P("tp", "tp2"), row_spec, P("tp2")), out_specs=(row_spec, row_spec), check_vma=False)
```

```python
import functools

import jax
import jax.numpy as jnp
from jax import lax
from jax.experimental import pallas as pl
from jax.experimental.pallas import tpu as pltpu
from jax.sharding import PartitionSpec as P

EPS_NORM = 1e-6
MESH = pl.DeviceIdType.MESH
F32, BF16 = jnp.float32, jnp.bfloat16

SPLIT = 1
NCH, NU, NY, NR, NE = 128 * SPLIT, 60 * SPLIT, 60 * SPLIT, 56 * SPLIT, 12 * SPLIT
LOOK, LAG = 6 * SPLIT, 3
CATCH, CAUGHT, AHEAD = 24 * SPLIT, 10, 4
TILE = 128
LOCAL = 256
STORE = 128


def gather_matmul(a, w, res, h, ss_out, asib, arem, wbuf, abuf, sbuf, rbuf, ss_own, ss_all,
                  ss_last, ss_lasts, ld, own_w, sib_recv, sib_send, y_recv, y_send, z_recv, z_send, e_recv, e_send, w_recv, w_send, ss_recv, ss_send, sl_recv, sl_send):
    x, z, t = lax.axis_index("dp"), lax.axis_index("tp2"), lax.axis_index("tp")
    rows, width = h.shape
    depth = w.shape[0]
    half = depth // 2
    ch = rows // NCH
    core, yy = lax.rem(t, 2), t // 2
    sib = yy * 2 + 1 - core
    far = (1 - yy) * 2
    zp = z + 1 - 2 * lax.rem(z, 2)
    middle = lax.rem((z + 1) // 2, 2)
    n_local = rows // LOCAL

    def aligned(v, m=ch):
        return pl.multiple_of(v, m)

    def y_row(zz, k):
        mid = lax.rem((zz + 1) // 2, 2)
        early = 1 - jnp.minimum(k // NE, 1)
        late = jnp.minimum(k // NR, 1)
        return (k + mid * (1 - late) * NU + mid * lax.rem(zz, 2) * early * NR) * ch

    def e_row(j):
        return (NU + (z // 2) * NR + j) * ch

    def y_send_to(k, r):
        row = y_row(z, k)
        return pltpu.make_async_remote_copy(
            src_ref=a.at[pl.ds(aligned((far + r) * rows + row), ch)], dst_ref=arem.at[pl.ds(aligned(core * rows + row), ch)],
            send_sem=y_send, recv_sem=y_recv.at[core, k], device_id=(x, z, far + r), device_id_type=MESH)

    def start_y(k):
        for r in range(2):
            y_send_to(k, r).start()

    def move(row, s, recv, k, send, dev):
        ref = arem.at[pl.ds(aligned(s * rows + row), ch)]
        return pltpu.make_async_remote_copy(src_ref=ref, dst_ref=ref, send_sem=send, recv_sem=recv.at[s, k], device_id=dev, device_id_type=MESH)

    def each(row, recv, k, send, dev, start):
        for s in range(2):
            c = move(row, s, recv, k, send, dev)
            c.start() if start else c.wait_recv()

    def wait_y(k):
        each(y_row(z, k), y_recv, k, z_send, (x, zp, t), False)

    def relay_z(k):
        each(y_row(z, k), z_recv, k, z_send, (x, zp, t), True)

    def wait_z(k):
        each(y_row(zp, k), z_recv, k, z_send, (x, zp, t), False)

    def w_move(slot, part, idx, dev, src=None):
        ref = wbuf.at[pl.ds(aligned(slot * depth + part * half, 128), half)]
        return pltpu.make_async_remote_copy(src_ref=ref if src is None else src, dst_ref=ref, send_sem=w_send.at[idx], recv_sem=w_recv.at[idx],
                                            device_id=dev, device_id_type=MESH)

    w_sib = pltpu.make_async_remote_copy(src_ref=w, dst_ref=wbuf.at[pl.ds(depth, depth)], send_sem=w_send.at[0], recv_sem=w_recv.at[0],
                                         device_id=(x, z, sib), device_id_type=MESH)
    w_y = w_move(2 + core, x, 1, (x, z, far + core), w.at[pl.ds(aligned(x * half, 128), half)])
    w_x = w_move(2 + core, x, 2, (1 - x, z, t))
    w_x_in = w_move(2 + core, 1 - x, 2, (1 - x, z, t))
    w_d0 = w_move(2 + core, x, 3, (x, z, sib))
    w_d1 = w_move(2 + core, 1 - x, 4, (x, z, sib))
    w_d0_in = w_move(3 - core, x, 3, (x, z, sib))
    w_d1_in = w_move(3 - core, 1 - x, 4, (x, z, sib))

    def sib_copy(i):
        return pltpu.make_async_remote_copy(
            src_ref=a.at[pl.ds(aligned(sib * rows + i * LOCAL), LOCAL)], dst_ref=asib.at[pl.ds(aligned(i * LOCAL), LOCAL)],
            send_sem=sib_send, recv_sem=sib_recv.at[i], device_id=(x, z, sib), device_id_type=MESH)

    def loads(i):
        slot = lax.rem(i, 2)
        here = pl.ds(aligned(i * LOCAL), LOCAL)
        return (pltpu.make_async_copy(a.at[pl.ds(aligned(t * rows + i * LOCAL), LOCAL)], abuf.at[slot], ld.at[slot, 0]),
                pltpu.make_async_copy(asib.at[here], sbuf.at[slot], ld.at[slot, 1]),
                pltpu.make_async_copy(res.at[here], rbuf.at[slot], ld.at[slot, 2]))

    def prefetch(i):
        sib_copy(i).wait_recv()
        for c in loads(i):
            c.start()

    def block(lhs, slot, cols):
        return jnp.dot(lhs, wbuf[pl.ds(slot * depth, depth), cols], preferred_element_type=F32).astype(BF16).astype(F32)

    def local_tile(i):
        slot = lax.rem(i, 2)
        for c in loads(i):
            c.wait()

        @pl.when(i + AHEAD < n_local)
        def _():
            sib_copy(i + AHEAD).start()

        @pl.when(i + 1 < n_local)
        def _():
            prefetch(i + 1)

        here = pl.ds(aligned(i * LOCAL), LOCAL)
        for n in range(width // 256):
            cols = pl.ds(n * 256, 256)
            h[here, cols] = rbuf[slot, :, cols].astype(F32) + block(abuf[slot], 0, cols) + block(sbuf[slot], 1, cols)

    def remote_tile(row):
        acc = jnp.zeros((TILE, 128), F32)
        here = pl.ds(aligned(row, TILE), TILE)
        there = pl.ds(aligned(rows + row, TILE), TILE)
        for n in range(width // 256):
            cols = pl.ds(n * 256, 256)
            v = h[here, cols] + block(arem[here, :], 2, cols) + block(arem[there, :], 3, cols)
            h[here, cols] = v
            sq = v * v
            acc = acc + sq[:, :128] + sq[:, 128:]
        return jnp.sum(acc.T, axis=0, keepdims=True)

    def tile(row):
        ss_own[pl.ds(row // TILE, 1), :] = remote_tile(row)

    cpt = TILE // ch

    def y_tile(i):
        tile(y_row(z, cpt * i))

    def z_wait(i):
        for s in range(cpt):
            wait_z(cpt * i + s)

    def z_tile(i):
        z_wait(i)
        tile(y_row(zp, cpt * i))

    barrier = pltpu.get_barrier_semaphore()
    partners = [(x, z, far), (x, z, far + 1), (x, z, sib), (1 - x, z, t)] + [(x, lax.rem(z + d, 4), t) for d in range(1, 4)]
    for dev in partners:
        pl.semaphore_signal(barrier, inc=1, device_id=dev, device_id_type=MESH)
    pl.semaphore_wait(barrier, len(partners))

    ss_own[...] = jnp.zeros_like(ss_own)
    for k in range(LOOK):
        start_y(k)
    own = pltpu.make_async_copy(w, wbuf.at[pl.ds(0, depth)], own_w)
    own.start()
    w_sib.start()
    for i in range(AHEAD):
        sib_copy(i).start()
    prefetch(0)
    own.wait()
    w_sib.wait_recv()

    def step(k):
        wait_y(k)

        @pl.when(k < NR)
        def _():
            relay_z(k)

        @pl.when(k + LOOK < NY)
        def _():
            start_y(k + LOOK)

    def first(k, c):
        step(k)

        @pl.when(middle == 1)
        def _():
            each(y_row(z, k), e_recv, k, e_send, (x, 3 - z, t), True)

        @pl.when(k == NE - 1 - LOOK)
        def _():
            w_y.start()

        @pl.when((middle == 1) & (k >= LAG))
        def _():
            swap(k - LAG)

        @pl.when(lax.rem(k, 2 * SPLIT) == 2 * SPLIT - 1)
        def _():
            local_tile(k // (2 * SPLIT))

        return c

    def extra(j):
        each(e_row(j), e_recv, j, e_send, (x, zp, t), False)

    def swap(j):
        extra(j)
        each(e_row(j), e_recv, j, e_send, (x, zp, t), True)

    lax.fori_loop(0, NE, first, 0)
    lax.fori_loop(NE - middle * LAG, NE, lambda j, c: (swap(j), c)[1], 0)
    lax.fori_loop(NE // (2 * SPLIT), n_local, lambda i, c: (local_tile(i), c)[1], 0)
    w_y.wait_recv()
    w_x.start()
    w_d0.start()
    lax.fori_loop(NE, CATCH, lambda k, c: (step(k), c)[1], 0)
    w_x_in.wait_recv()
    w_d1.start()
    w_d0_in.wait_recv()
    w_d1_in.wait_recv()

    def third(i, c):
        for s in range(SPLIT):
            step(CATCH + 2 * SPLIT * i + s)

        @pl.when(i == 0)
        def _():
            lax.fori_loop(middle * NE, NE, lambda j, c: (extra(j), c)[1], 0)
            lax.fori_loop(0, NE // cpt, lambda j, d: (tile(e_row(cpt * j)), d)[1], 0)

        y_tile(i)
        for s in range(SPLIT):
            step(CATCH + 2 * SPLIT * i + SPLIT + s)

        @pl.when(i < CAUGHT - 1)
        def _():
            z_tile(i)

        return c

    lax.fori_loop(0, CAUGHT, third, 0)

    def steps(lo, hi):
        lax.fori_loop(jnp.maximum(lo, CATCH + 2 * SPLIT * CAUGHT), jnp.minimum(hi, NY), lambda k, c: (step(k), c)[1], 0)

    def fourth(i, c):
        steps(cpt * i + 1, cpt * i + cpt)
        y_tile(i)
        steps(cpt * i + cpt, cpt * i + cpt + 1)
        z_tile(i - 1)
        return c

    lax.fori_loop(CAUGHT, NR // cpt, fourth, 0)
    def share(src, dst, send, recv):
        for d in range(1, 4):
            pltpu.make_async_remote_copy(src_ref=src, dst_ref=dst.at[z], send_sem=send.at[d], recv_sem=recv.at[z],
                                         device_id=(x, lax.rem(z + d, 4), t), device_id_type=MESH).start()

    def collect(src, dst, send, recv):
        for d in range(1, 4):
            zz = lax.rem(z + d, 4)
            pltpu.make_async_remote_copy(src_ref=src, dst_ref=dst.at[zz], send_sem=send.at[d], recv_sem=recv.at[zz],
                                         device_id=(x, zz, t), device_id_type=MESH).wait()
        dst[pl.ds(z, 1)] = src[...][None]
        return (dst[0] + dst[1]) + (dst[2] + dst[3])

    share(ss_own, ss_all, ss_send, ss_recv)
    steps(NR + 1, NY)

    n_pair = NR // cpt - 1
    in_first, in_second = n_pair, NU // cpt + n_pair
    ss_last[...] = jnp.zeros_like(ss_last)
    ss_last[pl.ds(0, 1), :] = remote_tile(NR * ch)
    ss_last[pl.ds(1 + middle, 1), :] = ss_own[pl.ds(y_row(z, n_pair * cpt) // TILE, 1), :]
    z_wait(n_pair)
    ss_last[pl.ds(2 - middle, 1), :] = remote_tile(y_row(zp, n_pair * cpt))
    share(ss_last, ss_lasts, sl_send, sl_recv)
    y_total = 2 * NY * ch
    pltpu.make_async_remote_copy(src_ref=a.at[pl.ds(0, y_total)], dst_ref=arem.at[pl.ds(0, y_total)], send_sem=y_send, recv_sem=y_recv.at[0, 0],
                                 device_id=(x, z, far), device_id_type=MESH).wait_send()
    z_total = 2 * NR * ch
    pltpu.make_async_remote_copy(src_ref=arem.at[pl.ds(0, z_total)], dst_ref=arem.at[pl.ds(0, z_total)], send_sem=z_send, recv_sem=z_recv.at[0, 0],
                                 device_id=(x, zp, t), device_id_type=MESH).wait_send()

    @pl.when(middle == 1)
    def _():
        n = 4 * NE * ch
        pltpu.make_async_remote_copy(src_ref=arem.at[pl.ds(0, n)], dst_ref=arem.at[pl.ds(0, n)], send_sem=e_send, recv_sem=e_recv.at[0, 0],
                                     device_id=(x, zp, t), device_id_type=MESH).wait_send()

    pltpu.make_async_remote_copy(src_ref=a.at[pl.ds(0, rows)], dst_ref=asib, send_sem=sib_send, recv_sem=sib_recv.at[0],
                                 device_id=(x, z, sib), device_id_type=MESH).wait_send()
    for c in (w_sib, w_y, w_x, w_d0, w_d1):
        c.wait_send()
    ss_out[...] = collect(ss_own, ss_all, ss_send, ss_recv)
    last = collect(ss_last, ss_lasts, sl_send, sl_recv)
    for j, row in enumerate((NR * ch // TILE, in_first, in_second)):
        ss_out[pl.ds(row, 1), :] = last[j:j + 1]


def normalize(total_cols, h, ss, gain, h_hbm, n_hbm, h_out, n_out, sem):
    n_blocks = h.shape[0] // STORE

    def out(i):
        here = pl.ds(pl.multiple_of(i * STORE, STORE), STORE)
        buf = pl.ds(pl.multiple_of(lax.rem(i, n_blocks // 2) * STORE, STORE), STORE)
        return (pltpu.make_async_copy(h_out.at[buf], h_hbm.at[here], sem.at[0, i]),
                pltpu.make_async_copy(n_out.at[buf], n_hbm.at[here], sem.at[1, i]))

    def start(i):
        for c in out(i):
            c.start()

    def wait(i):
        for c in out(i):
            c.wait()

    def block(i, carry):
        @pl.when(i >= n_blocks // 2)
        def _():
            wait(i - n_blocks // 2)

        for b in range(STORE // TILE):
            here = pl.ds(pl.multiple_of(i * STORE + b * TILE, TILE), TILE)
            to = pl.ds(pl.multiple_of(lax.rem(i, n_blocks // 2) * STORE + b * TILE, TILE), TILE)
            inv = lax.rsqrt(ss[pl.ds(i * (STORE // TILE) + b, 1), :] / total_cols + EPS_NORM)
            inv = jnp.broadcast_to(inv, (TILE, TILE)).T
            for c in range(h.shape[1] // 128):
                cols = pl.ds(c * 128, 128)
                v = h[here, cols]
                h_out[to, cols] = v.astype(BF16)
                n_out[to, cols] = (v * inv * gain[cols][None, :]).astype(BF16)

        @pl.when(i > 0)
        def _():
            start(i - 1)

        return carry

    lax.fori_loop(0, n_blocks, block, 0)
    start(n_blocks - 1)
    lax.fori_loop(n_blocks // 2, n_blocks, lambda i, c: (wait(i), c)[1], 0)


def solution(mesh):
    col_groups = mesh.shape["tp2"]
    n_tp = mesh.shape["tp"]

    def local_step(a, w, res, gain):
        rows, width = res.shape
        depth = w.shape[0]
        dma = pltpu.SemaphoreType.DMA
        h, ss, _ = pl.pallas_call(
            gather_matmul,
            out_shape=(pltpu.VMEM((rows, width), F32), pltpu.VMEM((rows // TILE, 128), F32),
                       jax.ShapeDtypeStruct((rows, depth), BF16)),
            in_specs=[pl.BlockSpec(memory_space=pl.ANY)] * 3,
            out_specs=(pl.BlockSpec(memory_space=pltpu.VMEM), pl.BlockSpec(memory_space=pltpu.VMEM), pl.BlockSpec(memory_space=pl.ANY)),
            scratch_shapes=[
                pltpu.VMEM((2 * rows, depth), BF16), pltpu.VMEM((n_tp * depth, width), BF16),
                pltpu.VMEM((2, LOCAL, depth), BF16), pltpu.VMEM((2, LOCAL, depth), BF16), pltpu.VMEM((2, LOCAL, width), BF16),
                pltpu.VMEM((rows // TILE, 128), F32), pltpu.VMEM((4, rows // TILE, 128), F32), pltpu.VMEM((8, 128), F32), pltpu.VMEM((4, 8, 128), F32),
                dma((2, 3)), dma, dma((rows // LOCAL,)), dma, dma((2, NY)), dma, dma((2, NY)), dma, dma((2, NE)), dma,
                dma((5,)), dma((5,)), dma((4,)), dma((4,)), dma((4,)), dma((4,)),
            ],
            compiler_params=pltpu.CompilerParams(collective_id=0, has_side_effects=True, vmem_limit_bytes=42 * 1024 * 1024),
            cost_estimate=pl.CostEstimate(flops=2 * rows * n_tp * depth * width, bytes_accessed=8 * rows * width, transcendentals=0),
            name="gather_matmul",
        )(a, w, res)
        return pl.pallas_call(
            functools.partial(normalize, width * col_groups),
            out_shape=(jax.ShapeDtypeStruct((rows, width), BF16),) * 2,
            in_specs=[pl.BlockSpec(memory_space=pltpu.VMEM)] * 3,
            out_specs=(pl.BlockSpec(memory_space=pl.ANY),) * 2,
            scratch_shapes=[pltpu.VMEM((rows // 2, width), BF16), pltpu.VMEM((rows // 2, width), BF16), dma((2, rows // STORE))],
            compiler_params=pltpu.CompilerParams(vmem_limit_bytes=14 * 1024 * 1024),
            name="normalize",
        )(h, ss, gain)

    row_spec = P(("dp", "tp"), "tp2")
    return jax.shard_map(local_step, mesh=mesh, in_specs=(P("dp", "tp"), P("tp", "tp2"), row_spec, P("tp2")), out_specs=(row_spec, row_spec), check_vma=False)
```
